32 devices in a mesh: dp: 1 (over z), tp: 4 (over y), cp: 8 (over x, core).
Axes of the slice: x: 4, y: 4, z: 1, core: 2. Of those that a mesh axis runs over, the one named last changes fastest.
The devices are a block of a 4x4x8 slice.
Arguments:
- x_in: bfloat16 [2, 4096, 3072], P('dp', 'cp')
- w_q: bfloat16 [3072, 24, 128], P(None, 'tp')
- w_k: bfloat16 [3072, 8, 128], P(None, 'tp')
- w_v: bfloat16 [3072, 8, 128], P(None, 'tp')
- w_o: bfloat16 [24, 128, 3072], P('tp')
- q_norm_w: float32 [24, 128], P('tp')
- k_norm_w: float32 [8, 128], P('tp')
- post_norm_w: float32 [3072], replicated
- grad_y: bfloat16 [2, 4096, 3072], P('dp', 'cp')
Outputs:
- output 1: bfloat16 [2, 4096, 3072], P('dp', 'cp')
- output 2: bfloat16 [2, 4096, 3072], P('dp', 'cp')
- output 3: float32 [3072, 24, 128], P('dp', 'tp')
- output 4: float32 [3072, 8, 128], P('dp', 'tp')
- output 5: float32 [3072, 8, 128], P('dp', 'tp')
- output 6: float32 [24, 128, 3072], P(('dp', 'tp'))
- output 7: float32 [24, 128], P(('dp', 'tp'))
- output 8: float32 [8, 128], P(('dp', 'tp'))
- output 9: float32 [3072], P('dp')
All inputs are finite; a program needn't handle non-finite values.
Results may differ from the reference program's by a relative error of at most 0.016555.
Values are sent between devices in bfloat16 or wider.
A program may use at most 768 MiB of HBM per device.

```python
import jax
import jax.numpy as jnp
from jax import lax

BATCH_SIZE = 2
SEQ_LEN = 4096
D_MODEL = 3072
NUM_HEADS = 24
KV_HEADS = 8
HEAD_DIM = 128
QUERY_ROWS = 256
ROPE_THETA = 500000.0
NORM_EPS = 1e-6


def setup_inputs(seed: int = 0, part: int = 0) -> dict:
    base_key = jax.random.key(seed)
    act_keys = jax.random.split(jax.random.fold_in(base_key, part), 2)
    wt_keys = jax.random.split(jax.random.fold_in(base_key, 1000003), 9)
    act_shape = (BATCH_SIZE, SEQ_LEN, D_MODEL)
    x_in = jax.random.normal(act_keys[0], act_shape, jnp.float32).astype(jnp.bfloat16)
    grad_y = jax.random.normal(act_keys[1], act_shape, jnp.float32).astype(jnp.bfloat16)
    in_scale = D_MODEL ** -0.5
    out_scale = (NUM_HEADS * HEAD_DIM) ** -0.5
    w_q = (jax.random.normal(wt_keys[0], (D_MODEL, NUM_HEADS, HEAD_DIM), jnp.float32) * in_scale).astype(jnp.bfloat16)
    w_k = (jax.random.normal(wt_keys[1], (D_MODEL, KV_HEADS, HEAD_DIM), jnp.float32) * in_scale).astype(jnp.bfloat16)
    w_v = (jax.random.normal(wt_keys[2], (D_MODEL, KV_HEADS, HEAD_DIM), jnp.float32) * in_scale).astype(jnp.bfloat16)
    w_o = (jax.random.normal(wt_keys[3], (NUM_HEADS, HEAD_DIM, D_MODEL), jnp.float32) * out_scale).astype(jnp.bfloat16)
    q_head_gain = jax.random.uniform(wt_keys[4], (NUM_HEADS, 1), jnp.float32, 0.6, 1.4)
    q_norm_w = q_head_gain * (1.0 + 0.1 * jax.random.normal(wt_keys[5], (NUM_HEADS, HEAD_DIM), jnp.float32))
    k_head_gain = jax.random.uniform(wt_keys[6], (KV_HEADS, 1), jnp.float32, 0.6, 1.4)
    k_norm_w = k_head_gain * (1.0 + 0.1 * jax.random.normal(wt_keys[7], (KV_HEADS, HEAD_DIM), jnp.float32))
    post_norm_w = 1.0 + 0.3 * jax.random.normal(wt_keys[8], (D_MODEL,), jnp.float32)
    return {"x_in": x_in, "w_q": w_q, "w_k": w_k, "w_v": w_v, "w_o": w_o, "q_norm_w": q_norm_w, "k_norm_w": k_norm_w, "post_norm_w": post_norm_w, "grad_y": grad_y}


def rope_tables():
    half_dim = HEAD_DIM // 2
    inv_freq = ROPE_THETA ** (-2.0 * jnp.arange(half_dim, dtype=jnp.float32) / HEAD_DIM)
    angles = jnp.arange(SEQ_LEN, dtype=jnp.float32)[:, None] * inv_freq[None, :]
    return jnp.cos(angles), jnp.sin(angles)


def apply_rope(values, cos_tab, sin_tab):
    half_dim = values.shape[-1] // 2
    low_half = values[..., :half_dim]
    high_half = values[..., half_dim:]
    cos_rows = cos_tab[:, None, :]
    sin_rows = sin_tab[:, None, :]
    return jnp.concatenate([low_half * cos_rows - high_half * sin_rows, high_half * cos_rows + low_half * sin_rows], axis=-1)


def whole_norm(lin_out, weight):
    inv_rms = lax.rsqrt(jnp.mean(lin_out * lin_out, axis=(-2, -1), keepdims=True) + NORM_EPS)
    return lin_out * inv_rms * weight


def causal_attention(q_rot, k_rot, v_val):
    group_size = NUM_HEADS // KV_HEADS
    n_blocks = SEQ_LEN // QUERY_ROWS
    q_heads = jnp.moveaxis(q_rot.reshape(BATCH_SIZE, SEQ_LEN, KV_HEADS, group_size, HEAD_DIM), 2, 0)
    k_heads = jnp.moveaxis(k_rot, 2, 0)
    v_heads = jnp.moveaxis(v_val, 2, 0)
    key_pos = jnp.arange(SEQ_LEN)
    score_scale = HEAD_DIM ** -0.5

    def one_head(head_args):
        q_head, k_head, v_head = head_args
        q_blocks = jnp.moveaxis(q_head.reshape(BATCH_SIZE, n_blocks, QUERY_ROWS, group_size, HEAD_DIM), 1, 0)

        def one_block(block_args):
            q_block, block_idx = block_args
            scores = jnp.einsum("bqgd,bkd->bgqk", q_block, k_head) * score_scale
            query_pos = block_idx * QUERY_ROWS + jnp.arange(QUERY_ROWS)
            allowed = query_pos[:, None] >= key_pos[None, :]
            scores = jnp.where(allowed, scores, -jnp.inf)
            probs_blk = jax.nn.softmax(scores, axis=-1)
            return jnp.einsum("bgqk,bkd->bqgd", probs_blk, v_head)

        out_blocks = lax.map(jax.checkpoint(one_block), (q_blocks, jnp.arange(n_blocks)))
        return jnp.moveaxis(out_blocks, 0, 1).reshape(BATCH_SIZE, SEQ_LEN, group_size, HEAD_DIM)

    out_heads = lax.map(one_head, (q_heads, k_heads, v_heads))
    return jnp.moveaxis(out_heads, 0, 2).reshape(BATCH_SIZE, SEQ_LEN, NUM_HEADS, HEAD_DIM)


def forward(x_f, w_q, w_k, w_v, w_o, q_norm_w, k_norm_w, post_norm_w):
    cos_tab, sin_tab = rope_tables()
    q_lin = jnp.einsum("btd,dhe->bthe", x_f, w_q)
    k_lin = jnp.einsum("btd,dhe->bthe", x_f, w_k)
    v_lin = jnp.einsum("btd,dhe->bthe", x_f, w_v)
    q_rot = apply_rope(whole_norm(q_lin, q_norm_w), cos_tab, sin_tab).astype(jnp.bfloat16).astype(jnp.float32)
    k_rot = apply_rope(whole_norm(k_lin, k_norm_w), cos_tab, sin_tab).astype(jnp.bfloat16).astype(jnp.float32)
    v_val = v_lin.astype(jnp.bfloat16).astype(jnp.float32)
    attn_out = causal_attention(q_rot, k_rot, v_val).astype(jnp.bfloat16).astype(jnp.float32)
    proj = jnp.einsum("bthe,hed->btd", attn_out, w_o)
    post_hat = proj * lax.rsqrt(jnp.mean(proj * proj, axis=-1, keepdims=True) + NORM_EPS)
    return x_f + post_hat * post_norm_w


def reference(x_in, w_q, w_k, w_v, w_o, q_norm_w, k_norm_w, post_norm_w, grad_y):
    y_full, pullback = jax.vjp(forward, x_in.astype(jnp.float32), w_q.astype(jnp.float32), w_k.astype(jnp.float32), w_v.astype(jnp.float32), w_o.astype(jnp.float32), q_norm_w, k_norm_w, post_norm_w)
    all_grads = pullback(grad_y.astype(jnp.float32))
    return (y_full.astype(jnp.bfloat16), all_grads[0].astype(jnp.bfloat16), all_grads[1], all_grads[2], all_grads[3], all_grads[4], all_grads[5], all_grads[6], all_grads[7])
```

```python
import functools

import jax
import jax.numpy as jnp
from jax import lax
from jax.experimental import pallas as pl
from jax.experimental.pallas import tpu as pltpu
from jax.sharding import PartitionSpec as P

ROPE_THETA = 500000.0
NORM_EPS = 1e-6
MASK_VALUE = -1e30
LOG2E = 1.4426950408889634
NT = (((1,), (1,)), ((), ()))
NN = (((1,), (0,)), ((), ()))
TN = (((0,), (0,)), ((), ()))


def rope_tables(start_pos, seq_rows, head_dim):
    half_dim = head_dim // 2
    inv_freq = ROPE_THETA ** (-2.0 * jnp.arange(half_dim, dtype=jnp.float32) / head_dim)
    positions = (start_pos + jnp.arange(seq_rows)).astype(jnp.float32)
    angles = positions[:, None] * inv_freq[None, :]
    return jnp.cos(angles), jnp.sin(angles)


def apply_rope(values, cos_tab, sin_tab):
    half_dim = values.shape[-1] // 2
    low_half = values[..., :half_dim]
    high_half = values[..., half_dim:]
    cos_rows = cos_tab[:, None, :]
    sin_rows = sin_tab[:, None, :]
    return jnp.concatenate([low_half * cos_rows - high_half * sin_rows, high_half * cos_rows + low_half * sin_rows], axis=-1)


def rope_back(grad_in, cos_tab, sin_tab):
    return apply_rope(grad_in, cos_tab, -sin_tab)


def dot32(lhs, rhs, dims):
    return lax.dot_general(lhs, rhs, dims, preferred_element_type=jnp.float32)


def attend_kernel(n_group, score_scale, q_ref, k_ref, v_ref, o_ref, lse_ref, acc_ref, max_ref):
    block_len = q_ref.shape[0]
    dim = k_ref.shape[2]
    me = lax.axis_index("cp")
    to_log2 = score_scale * LOG2E
    n_rep = block_len // dim

    def one_block(blk, first):
        k_blk = k_ref[blk]
        v_ext = jnp.concatenate([v_ref[blk], jnp.ones((block_len, dim), jnp.bfloat16)], axis=1)
        for grp in range(n_group):
            q_grp = q_ref[:, grp * dim:(grp + 1) * dim]
            scores = dot32(q_grp, k_blk, NT) * to_log2
            if first:
                rows = lax.broadcasted_iota(jnp.int32, scores.shape, 0)
                cols = lax.broadcasted_iota(jnp.int32, scores.shape, 1)
                scores = jnp.where(rows >= cols, scores, MASK_VALUE)
                new_max = jnp.broadcast_to(jnp.max(scores, axis=1, keepdims=True), (block_len, dim))
                prob = jnp.exp2(scores - jnp.concatenate([new_max] * n_rep, axis=1))
                acc_ref[grp] = dot32(prob.astype(jnp.bfloat16), v_ext, NN)
            else:
                old_max = max_ref[grp]
                new_max = jnp.maximum(old_max, jnp.broadcast_to(jnp.max(scores, axis=1, keepdims=True), (block_len, dim)))
                prob = jnp.exp2(scores - jnp.concatenate([new_max] * n_rep, axis=1))
                rescale = jnp.exp2(old_max - new_max)
                acc_ref[grp] = (acc_ref[grp] * jnp.concatenate([rescale, rescale], axis=1)
                                + dot32(prob.astype(jnp.bfloat16), v_ext, NN))
            max_ref[grp] = new_max

    one_block(me, True)

    def step(blk, carry):
        one_block(blk, False)
        return carry

    lax.fori_loop(0, me, step, 0)
    for grp in range(n_group):
        row_sum = acc_ref[grp, :, dim:]
        o_ref[:, grp * dim:(grp + 1) * dim] = (acc_ref[grp, :, :dim] / row_sum).astype(jnp.bfloat16)
        lse = jnp.transpose(max_ref[grp] + jnp.log2(row_sum))
        lse_ref[0, grp:grp + 1, :] = lse[0:1, :]


def attend_back_kernel(n_group, score_scale, q_ref, do_ref, o_ref, lse_ref, k_ref, v_ref, dq_ref, dk_ref, dv_ref, delta_ref):
    block_len = q_ref.shape[0]
    dim = k_ref.shape[2]
    n_blocks = k_ref.shape[0]
    me = lax.axis_index("cp")
    to_log2 = score_scale * LOG2E
    for grp in range(n_group):
        lanes = slice(grp * dim, (grp + 1) * dim)
        prod = do_ref[:, lanes].astype(jnp.float32) * o_ref[:, lanes].astype(jnp.float32)
        delta_ref[grp:grp + 1, :] = jnp.sum(jnp.transpose(prod), axis=0, keepdims=True)

    def one_block(blk, first):
        k_blk = k_ref[blk]
        v_blk = v_ref[blk]
        dk_sum = None
        dv_sum = None
        for grp in range(n_group):
            lanes = slice(grp * dim, (grp + 1) * dim)
            q_grp = q_ref[:, lanes]
            do_grp = do_ref[:, lanes]
            scores = dot32(k_blk, q_grp, NT) * to_log2
            if first:
                rows = lax.broadcasted_iota(jnp.int32, scores.shape, 0)
                cols = lax.broadcasted_iota(jnp.int32, scores.shape, 1)
                scores = jnp.where(cols >= rows, scores, MASK_VALUE)
            prob = jnp.exp2(scores - lse_ref[0, grp:grp + 1, :])
            grad_p = dot32(v_blk, do_grp, NT)
            grad_s = (prob * (grad_p - delta_ref[grp:grp + 1, :])).astype(jnp.bfloat16)
            dv_part = dot32(prob.astype(jnp.bfloat16), do_grp, NN)
            dk_part = dot32(grad_s, q_grp, NN)
            dq_part = dot32(grad_s, k_blk, TN)
            dv_sum = dv_part if dv_sum is None else dv_sum + dv_part
            dk_sum = dk_part if dk_sum is None else dk_sum + dk_part
            if first:
                dq_ref[:, lanes] = dq_part
            else:
                dq_ref[:, lanes] += dq_part
        dk_ref[blk] = dk_sum * score_scale
        dv_ref[blk] = dv_sum

    one_block(me, True)

    def step(blk, carry):
        one_block(blk, False)
        return carry

    lax.fori_loop(0, me, step, 0)
    dq_ref[...] = dq_ref[...] * score_scale

    def clear(blk, carry):
        dk_ref[blk] = jnp.zeros((block_len, dim), jnp.float32)
        dv_ref[blk] = jnp.zeros((block_len, dim), jnp.float32)
        return carry

    lax.fori_loop(me + 1, n_blocks, clear, 0)


def attend(q_rot, kv_all, kv_loc, n_group, dim, score_scale):
    block_len, q_cols = q_rot.shape
    n_blocks = kv_all.shape[0]
    wide = n_group * dim
    pairs = kv_loc * n_group * n_blocks * block_len * block_len
    return pl.pallas_call(
        functools.partial(attend_kernel, n_group, score_scale),
        grid=(kv_loc,),
        in_specs=[
            pl.BlockSpec((block_len, wide), lambda h: (0, h)),
            pl.BlockSpec((n_blocks, block_len, dim), lambda h: (0, 0, h)),
            pl.BlockSpec((n_blocks, block_len, dim), lambda h: (0, 0, kv_loc + h)),
        ],
        out_specs=[
            pl.BlockSpec((block_len, wide), lambda h: (0, h)),
            pl.BlockSpec((1, n_group, block_len), lambda h: (h, 0, 0)),
        ],
        out_shape=[
            jax.ShapeDtypeStruct((block_len, q_cols), jnp.bfloat16),
            jax.ShapeDtypeStruct((kv_loc, n_group, block_len), jnp.float32),
        ],
        scratch_shapes=[
            pltpu.VMEM((n_group, block_len, 2 * dim), jnp.float32),
            pltpu.VMEM((n_group, block_len, dim), jnp.float32),
        ],
        compiler_params=pltpu.CompilerParams(vmem_limit_bytes=40 * 1024 * 1024),
        cost_estimate=pl.CostEstimate(flops=8 * pairs * dim, bytes_accessed=2 * kv_all.size, transcendentals=pairs),
        name="attend",
    )(q_rot, kv_all, kv_all)


def attend_back(q_rot, grad_o, attn_out, lse, kv_all, kv_loc, n_group, dim, score_scale):
    block_len, q_cols = q_rot.shape
    n_blocks = kv_all.shape[0]
    wide = n_group * dim
    pairs = kv_loc * n_group * n_blocks * block_len * block_len
    q_spec = pl.BlockSpec((block_len, wide), lambda h: (0, h))
    k_spec = pl.BlockSpec((n_blocks, block_len, dim), lambda h: (0, 0, h))
    return pl.pallas_call(
        functools.partial(attend_back_kernel, n_group, score_scale),
        grid=(kv_loc,),
        in_specs=[
            q_spec, q_spec, q_spec,
            pl.BlockSpec((1, n_group, block_len), lambda h: (h, 0, 0)),
            k_spec,
            pl.BlockSpec((n_blocks, block_len, dim), lambda h: (0, 0, kv_loc + h)),
        ],
        out_specs=[q_spec, k_spec, k_spec],
        out_shape=[
            jax.ShapeDtypeStruct((block_len, q_cols), jnp.float32),
            jax.ShapeDtypeStruct((n_blocks, block_len, kv_loc * dim), jnp.float32),
            jax.ShapeDtypeStruct((n_blocks, block_len, kv_loc * dim), jnp.float32),
        ],
        scratch_shapes=[pltpu.VMEM((n_group, block_len), jnp.float32)],
        compiler_params=pltpu.CompilerParams(vmem_limit_bytes=48 * 1024 * 1024),
        cost_estimate=pl.CostEstimate(flops=20 * pairs * dim, bytes_accessed=4 * kv_all.size, transcendentals=pairs),
        name="attend_back",
    )(q_rot, grad_o, attn_out, lse, kv_all, kv_all)


def solution(mesh):
    tp_size = mesh.shape["tp"]
    cp_size = mesh.shape["cp"]
    tp_next = [(dev, (dev + 1) % tp_size) for dev in range(tp_size)]
    tp_prev = [(dev, (dev + tp_size - 1) % tp_size) for dev in range(tp_size)]
    swap_core = [(dev, dev ^ 1) for dev in range(cp_size)]
    act_spec = P("dp", "cp", None)
    col_spec = P(None, "tp", None)
    part_col = P("dp", "tp", None)
    in_specs = (act_spec, col_spec, col_spec, col_spec, P("tp", None, None), P("tp", None), P("tp", None), P(None), act_spec)
    out_specs = (act_spec, act_spec, part_col, part_col, part_col, P(("dp", "tp"), None, None), P(("dp", "tp"), None), P(("dp", "tp"), None), P("dp"))

    def gather_tp_rows(w_loc, core):
        half_rows = w_loc.shape[0] // 2
        quarter = half_rows // 2
        mine = lax.dynamic_slice_in_dim(w_loc, core * half_rows, half_rows, 0)
        lower = lax.ppermute(mine, "tp", tp_next)
        upper = lax.ppermute(mine, "tp", tp_prev)
        far_a = lax.ppermute(lower[:quarter], "tp", tp_next)
        far_b = lax.ppermute(upper[quarter:], "tp", tp_prev)
        out = []
        for got in (lower, upper, jnp.concatenate([far_a, far_b], axis=0)):
            other = lax.ppermute(got, "cp", swap_core)
            out.append(jnp.where(core == 0, jnp.concatenate([got, other], axis=0), jnp.concatenate([other, got], axis=0)))
        return out

    def local_run(x_in, w_q, w_k, w_v, w_o, q_norm_w, k_norm_w, post_norm_w, grad_y):
        n_batch, block_len, width = x_in.shape
        heads_loc = w_q.shape[1]
        kv_loc = w_k.shape[1]
        dim = w_q.shape[2]
        n_group = heads_loc // kv_loc
        q_cols = heads_loc * dim
        k_cols = kv_loc * dim
        q_width = q_cols * tp_size
        k_width = k_cols * tp_size
        score_scale = dim ** -0.5
        cp_index = lax.axis_index("cp")
        tp_index = lax.axis_index("tp")
        core = lax.rem(cp_index, 2)
        cos_tab, sin_tab = rope_tables(cp_index * block_len, block_len, dim)
        w_o2 = w_o.reshape(q_cols, width)
        wo_parts = [w_o2] + gather_tp_rows(w_o2, core)

        q_lin = jnp.einsum("bld,dhe->blhe", x_in, w_q, preferred_element_type=jnp.float32)
        k_lin = jnp.einsum("bld,dhe->blhe", x_in, w_k, preferred_element_type=jnp.float32)
        v_lin = jnp.einsum("bld,dhe->blhe", x_in, w_v, preferred_element_type=jnp.float32)
        sums = jnp.stack([jnp.sum(q_lin * q_lin, axis=(2, 3)), jnp.sum(k_lin * k_lin, axis=(2, 3))])
        sums = lax.psum(sums, "tp")
        q_inv = lax.rsqrt(sums[0] / q_width + NORM_EPS)[:, :, None, None]
        k_inv = lax.rsqrt(sums[1] / k_width + NORM_EPS)[:, :, None, None]
        q_hat = q_lin * q_inv
        k_hat = k_lin * k_inv
        k_rot = apply_rope(k_hat * k_norm_w, cos_tab, sin_tab).astype(jnp.bfloat16).reshape(n_batch, block_len, k_cols)
        v_val = v_lin.astype(jnp.bfloat16).reshape(n_batch, block_len, k_cols)
        q_rot = apply_rope(q_hat * q_norm_w, cos_tab, sin_tab).astype(jnp.bfloat16).reshape(n_batch, block_len, q_cols)
        kv_own = jnp.concatenate([k_rot, v_val], axis=2)
        kv_all = [lax.all_gather(kv_own[b], "cp") for b in range(n_batch)]

        y_list, gproj_list, o_list, lse_list, gpost_list = [], [], [], [], []
        for b in range(n_batch):
            attn_out, lse = attend(q_rot[b], kv_all[b], kv_loc, n_group, dim, score_scale)
            o_list.append(attn_out)
            lse_list.append(lse)
        for b in range(n_batch):
            o_all = lax.all_gather(o_list[b], "tp")
            proj = dot32(o_list[b], wo_parts[0], NN)
            for part, shift in ((1, tp_size - 1), (2, 1), (3, 2)):
                o_part = lax.dynamic_index_in_dim(o_all, lax.rem(tp_index + shift, tp_size), 0, keepdims=False)
                proj = proj + dot32(o_part, wo_parts[part], NN)
            post_inv = lax.rsqrt(jnp.mean(proj * proj, axis=-1, keepdims=True) + NORM_EPS)
            post_hat = proj * post_inv
            y_list.append((x_in[b] + post_hat * post_norm_w).astype(jnp.bfloat16))
            grad_f = grad_y[b].astype(jnp.float32)
            gpost_list.append(jnp.sum(grad_f * post_hat, axis=0))
            grad_hat = grad_f * post_norm_w
            gproj_list.append((post_inv * (grad_hat - post_hat * jnp.mean(grad_hat * post_hat, axis=-1, keepdims=True))).astype(jnp.bfloat16))
        y_out = jnp.stack(y_list)
        grad_post = gpost_list[0]
        for term in gpost_list[1:]:
            grad_post = grad_post + term

        gq_list, gk_list, gv_list, gqn, gkn = [], [], [], 0.0, 0.0
        dx_list = []
        for b in range(n_batch):
            grad_o = dot32(gproj_list[b], w_o2, NT).astype(jnp.bfloat16)
            dq_rot, dk_all, dv_all = attend_back(q_rot[b], grad_o, o_list[b], lse_list[b], kv_all[b], kv_loc, n_group, dim, score_scale)
            dkv = lax.psum_scatter(jnp.concatenate([dk_all, dv_all], axis=2), "cp", scatter_dimension=0, tiled=False)
            dk_rot = dkv[:, :k_cols].reshape(block_len, kv_loc, dim)
            grad_v16 = dkv[:, k_cols:].astype(jnp.bfloat16)
            grad_q = rope_back(dq_rot.reshape(block_len, heads_loc, dim), cos_tab, sin_tab)
            grad_k = rope_back(dk_rot, cos_tab, sin_tab)
            gqn = gqn + jnp.sum(grad_q * q_hat[b], axis=0)
            gkn = gkn + jnp.sum(grad_k * k_hat[b], axis=0)
            grad_q = grad_q * q_norm_w
            grad_k = grad_k * k_norm_w
            dots = lax.psum(jnp.stack([jnp.sum(grad_q * q_hat[b], axis=(1, 2)), jnp.sum(grad_k * k_hat[b], axis=(1, 2))]), "tp")
            grad_q16 = (q_inv[b] * (grad_q - q_hat[b] * (dots[0] / q_width)[:, None, None])).astype(jnp.bfloat16)
            grad_k16 = (k_inv[b] * (grad_k - k_hat[b] * (dots[1] / k_width)[:, None, None])).astype(jnp.bfloat16)
            grad_v16 = grad_v16.reshape(block_len, kv_loc, dim)
            dx_part = (jnp.einsum("lhe,dhe->ld", grad_q16, w_q, preferred_element_type=jnp.float32)
                       + jnp.einsum("lhe,dhe->ld", grad_k16, w_k, preferred_element_type=jnp.float32)
                       + jnp.einsum("lhe,dhe->ld", grad_v16, w_v, preferred_element_type=jnp.float32))
            dx_own = lax.psum_scatter(dx_part, "tp", scatter_dimension=0, tiled=True)
            rows = dx_own.shape[0]
            gy_own = lax.dynamic_slice_in_dim(grad_y[b], tp_index * rows, rows, 0).astype(jnp.float32)
            dx_list.append(lax.all_gather((gy_own + dx_own).astype(jnp.bfloat16), "tp", tiled=True))
            gq_list.append(grad_q16)
            gk_list.append(grad_k16)
            gv_list.append(grad_v16)
        grad_x = jnp.stack(dx_list)
        grad_w_o = lax.psum(jnp.einsum("ble,bld->ed", jnp.stack(o_list), jnp.stack(gproj_list), preferred_element_type=jnp.float32), "cp")
        grad_w_q = jnp.einsum("bld,blhe->dhe", x_in, jnp.stack(gq_list), preferred_element_type=jnp.float32)
        grad_w_k = jnp.einsum("bld,blhe->dhe", x_in, jnp.stack(gk_list), preferred_element_type=jnp.float32)
        grad_w_v = jnp.einsum("bld,blhe->dhe", x_in, jnp.stack(gv_list), preferred_element_type=jnp.float32)
        grad_w_q, grad_w_k, grad_w_v, gqn, gkn, grad_post = lax.psum((grad_w_q, grad_w_k, grad_w_v, gqn, gkn, grad_post), "cp")
        return (y_out, grad_x, grad_w_q, grad_w_k, grad_w_v, grad_w_o.reshape(heads_loc, dim, width), gqn, gkn, grad_post)

    return jax.shard_map(local_run, mesh=mesh, in_specs=in_specs, out_specs=out_specs, check_vma=False)
```
